32 devices in a mesh: dp: 8 (over z, y), tensor: 4 (over x, core).
Axes of the slice: x: 2, y: 2, z: 4, core: 2. Of those that a mesh axis runs over, the one named last changes fastest.
Arguments:
- layer_outs: bfloat16 [5, 8192, 4096], P(None, 'dp', 'tensor'), may hold values from -6 to 6
- avg_grads: bfloat16 [4, 8192, 4096], P(None, 'dp', 'tensor'), may hold values from -0.0010299683 to 0.0010299683
- attn_mixed: bfloat16 [8192, 4096], P('dp', 'tensor'), may hold values from -96 to 96
- dwa_coefs: float32 [4, 5], replicated, may hold values from -1.5 to 1.5
Outputs:
- coef_grad: float32 [4, 5], replicated
- proj_grad: float32 [4096, 4096], P('dp', 'tensor')
The draws below stay inside these ranges and needn't reach their ends.
All inputs are finite; a program needn't handle non-finite values.
Results may differ from the reference program's by a relative error of at most 0.0042.
Values may be sent and summed in bfloat16 or wider, within the bound.
A program may use at most 128 MiB of HBM per device.

```python
import jax
import jax.numpy as jnp
from jax import lax

D = 4096
LAYERS = 4
TOKENS = 8192


def steps_of(rng, dims, split, least, largest):
    factor_of, own = 1.0, jax.random.fold_in(rng, 6)
    for dim, blocks in split:
        heights = jnp.exp(jax.random.uniform(jax.random.fold_in(own, dim), (blocks,), jnp.float32, least / len(split), largest / len(split)))
        factor_of = factor_of * jnp.repeat(heights, dims[dim] // blocks).reshape([-1 if axis == dim else 1 for axis in range(len(dims))])
    return factor_of


def bell_draw(own_key, dims, scale, bound, split=(), kind=jnp.bfloat16):
    array = scale * jax.random.normal(own_key, dims, jnp.float32)
    if split:
        array = array * steps_of(own_key, dims, split, -0.22, 0.18)
    return jnp.clip(array, -bound, bound).astype(kind)


def setup_inputs(seed: int = 0) -> dict:
    keys = jax.random.split(jax.random.key(seed), 5)
    layer_outs = bell_draw(keys[0], (LAYERS + 1, TOKENS, D), 1.0, 6.0, ((1, 8), (2, 4)))
    avg_grads = bell_draw(keys[1], (LAYERS, TOKENS, D), (1.0 / (TOKENS * D) ** 0.5), 0.0010299683, ((1, 8), (2, 4)))
    attn_mixed = bell_draw(keys[2], (TOKENS, D), (D ** 0.5 / 4), 96.0, ((0, 8), (1, 4)))
    dwa_coefs = jnp.clip(jax.random.uniform(keys[3], (LAYERS, LAYERS + 1), jnp.float32, -1.5, 1.5), -1.5, 1.5)
    return dict(layer_outs=layer_outs, avg_grads=avg_grads, attn_mixed=attn_mixed, dwa_coefs=dwa_coefs)


def reference(layer_outs, avg_grads, attn_mixed, dwa_coefs):
    grads_flat = avg_grads.reshape(LAYERS, -1)
    outs_flat = layer_outs.reshape(LAYERS + 1, -1)
    raw = lax.dot_general(grads_flat, outs_flat, (((1,), (1,)), ((), ())), preferred_element_type=jnp.float32)
    rows = jnp.arange(LAYERS, dtype=jnp.int32)[:, None]
    cols = jnp.arange(LAYERS + 1, dtype=jnp.int32)[None, :]
    coef_grad = jnp.where(cols <= rows + 1, raw, jnp.float32(0.0))
    first = dwa_coefs[LAYERS - 2, LAYERS - 1] * avg_grads[LAYERS - 2].astype(jnp.float32)
    second = dwa_coefs[LAYERS - 1, LAYERS - 1] * avg_grads[LAYERS - 1].astype(jnp.float32)
    out_grad = (first + second).astype(jnp.bfloat16)
    proj_grad = lax.dot_general(out_grad, attn_mixed, (((0,), (0,)), ((), ())), preferred_element_type=jnp.float32)
    return coef_grad, proj_grad
```

```python
import functools

import jax
import jax.numpy as jnp
from jax import lax
from jax.experimental import pallas as pl
from jax.experimental.pallas import tpu as pltpu
from jax.sharding import PartitionSpec as P

CHUNKS = 4
LANES = 128


def kernel(
    dp_size, tensor_size, outs_hbm, grads_hbm, attn_hbm, coefs, coef_out, proj_out,
    outs, grads, attn, gathered, y_send, y_recv, own, z_left, z_right, coef_a, coef_b,
    load_sem, g_send, x_send, g_recv, y_send_sem, y_recv_sem,
    z_send_sem, zl_sem, zr_sem, ca_send, ca_recv, cb_send, cb_recv,
):
    depth, tokens, features = grads.shape
    rows, cols = proj_out.shape
    ys = dp_size // tensor_size
    zs = tensor_size
    xs = tensor_size // 2
    chunk = rows // CHUNKS
    dp, tensor = lax.axis_index("dp"), lax.axis_index("tensor")
    z, y = dp // ys, dp % ys
    x, core = tensor // 2, tensor % 2
    partner = x * 2 + 1 - core

    loads = []
    order = [depth - 2, depth - 1]
    for i in order:
        loads.append(pltpu.make_async_copy(grads_hbm.at[i], grads.at[i], load_sem.at[i]))
    loads.append(pltpu.make_async_copy(attn_hbm, attn, load_sem.at[depth]))
    for i in range(depth - 2):
        loads.append(pltpu.make_async_copy(grads_hbm.at[i], grads.at[i], load_sem.at[i]))
    for j in range(depth + 1):
        loads.append(pltpu.make_async_copy(outs_hbm.at[j], outs.at[j], load_sem.at[depth + 1 + j]))
    for load in loads:
        load.start()

    barrier = pltpu.get_barrier_semaphore()
    for i in range(1, tensor_size):
        pl.semaphore_signal(
            barrier, inc=1, device_id={"tensor": (tensor + i) % tensor_size},
            device_id_type=pl.DeviceIdType.MESH,
        )
    for i in range(1, dp_size):
        pl.semaphore_signal(
            barrier, inc=1, device_id={"dp": (dp + i) % dp_size},
            device_id_type=pl.DeviceIdType.MESH,
        )
    pl.semaphore_wait(barrier, tensor_size + dp_size - 2)

    def piece(slot, part):
        return gathered.at[slot, pl.ds(pl.multiple_of(part * rows, rows), rows), :]

    def to_partner(slot, part):
        return pltpu.make_async_remote_copy(
            src_ref=piece(slot, part), dst_ref=piece(slot, part),
            send_sem=g_send.at[slot // 2, part], recv_sem=g_recv.at[slot, part],
            device_id={"tensor": partner}, device_id_type=pl.DeviceIdType.MESH,
        )

    def to_x(other, part):
        return pltpu.make_async_remote_copy(
            src_ref=piece(tensor, part), dst_ref=piece(tensor, part),
            send_sem=x_send.at[other, part], recv_sem=g_recv.at[tensor, part],
            device_id={"tensor": other * 2 + core}, device_id_type=pl.DeviceIdType.MESH,
        )

    def arrive(slot, part):
        pltpu.make_async_remote_copy(
            src_ref=piece(slot, part), dst_ref=piece(slot, part),
            send_sem=g_send.at[slot // 2, part], recv_sem=g_recv.at[slot, part],
            device_id={"tensor": partner}, device_id_type=pl.DeviceIdType.MESH,
        ).wait_recv()

    def make(part):
        first, second = coefs[depth - 2, depth - 1], coefs[depth - 1, depth - 1]

        @pl.loop(0, tokens // LANES)
        def _(step):
            at = pl.ds(pl.multiple_of(step * LANES, LANES), LANES)
            wide = pl.ds(pl.multiple_of(part * rows, LANES), rows)
            value = first * grads[depth - 2, at, wide].astype(jnp.float32)
            value += second * grads[depth - 1, at, wide].astype(jnp.float32)
            into = pl.ds(pl.multiple_of(part * rows, rows), rows)
            gathered[tensor, into, at] = value.T.astype(jnp.bfloat16)

        to_partner(tensor, part).start()
        for i in range(1, xs):
            to_x((x + i) % xs, part).start()

    def block(slot, part, k):
        at = pl.ds(pl.multiple_of(part * rows + k * chunk, chunk), chunk)
        return jnp.dot(gathered[slot, at, :], attn[...], preferred_element_type=jnp.float32)

    def strip(k):
        return pl.ds(pl.multiple_of(k * chunk, chunk), chunk)

    def y_copy(slot, i, k):
        return pltpu.make_async_remote_copy(
            src_ref=y_send.at[i - 1, slot, strip(k), :], dst_ref=y_recv.at[i - 1, slot, strip(k), :],
            send_sem=y_send_sem.at[i - 1, slot, k], recv_sem=y_recv_sem.at[i - 1, slot, k],
            device_id={"dp": z * ys + (y + i) % ys}, device_id_type=pl.DeviceIdType.MESH,
        )

    def y_start(slot):
        for i in range(1, ys):
            @pl.loop(0, CHUNKS)
            def _(k):
                y_send[i - 1, slot, strip(k), :] = block(slot, (y + i) % ys, k).astype(jnp.bfloat16)
                y_copy(slot, i, k).start()

    def keep(slot):
        @pl.loop(0, CHUNKS)
        def _(k):
            own[slot, strip(k), :] = block(slot, y, k)

    def right_copy(slot, k):
        return pltpu.make_async_remote_copy(
            src_ref=y_send.at[0, slot, strip(k), :], dst_ref=z_left.at[slot, strip(k), :],
            send_sem=z_send_sem.at[slot, k], recv_sem=zl_sem.at[slot, k],
            device_id={"dp": dp + ys}, device_id_type=pl.DeviceIdType.MESH,
        )

    def left_copy(slot, k):
        return pltpu.make_async_remote_copy(
            src_ref=y_send.at[0, slot, strip(k), :], dst_ref=z_right.at[slot, strip(k), :],
            send_sem=z_send_sem.at[slot, k], recv_sem=zr_sem.at[slot, k],
            device_id={"dp": dp - ys}, device_id_type=pl.DeviceIdType.MESH,
        )

    def pass_on(slot):
        @pl.loop(0, CHUNKS)
        def _(k):
            total = own[slot, strip(k), :]
            for i in range(1, ys):
                y_copy(slot, i, k).wait_send()
                y_copy(slot, i, k).wait_recv()
                total += y_recv[i - 1, slot, strip(k), :].astype(jnp.float32)
            own[slot, strip(k), :] = total

            @pl.when(slot > z)
            def _():
                @pl.when(z > 0)
                def _():
                    right_copy(slot, k).wait_recv()
                    own[slot, strip(k), :] += z_left[slot, strip(k), :].astype(jnp.float32)

                y_send[0, slot, strip(k), :] = own[slot, strip(k), :].astype(jnp.bfloat16)
                right_copy(slot, k).start()

            @pl.when(slot < z)
            def _():
                @pl.when(z < zs - 1)
                def _():
                    left_copy(slot, k).wait_recv()
                    own[slot, strip(k), :] += z_right[slot, strip(k), :].astype(jnp.float32)

                y_send[0, slot, strip(k), :] = own[slot, strip(k), :].astype(jnp.bfloat16)
                left_copy(slot, k).start()

    def coef_partial():
        pairs = [(i, j) for i in range(depth) for j in range(min(i + 2, depth + 1))]

        def step(r, sums):
            at = pl.ds(pl.multiple_of(r * 16, 16), 16)
            sums = list(sums)
            for col in range(features // LANES):
                lanes = slice(col * LANES, (col + 1) * LANES)
                g = [grads[i, at, lanes].astype(jnp.float32) for i in range(depth)]
                o = [outs[j, at, lanes].astype(jnp.float32) for j in range(depth + 1)]
                for n, (i, j) in enumerate(pairs):
                    product = g[i] * o[j]
                    sums[n] += product[:8] + product[8:]
            return tuple(sums)

        zero = jnp.zeros((8, LANES), jnp.float32)
        sums = lax.fori_loop(0, tokens // 16, step, tuple(zero for _ in pairs))
        row = lax.broadcasted_iota(jnp.int32, (8, LANES), 0)
        col = lax.broadcasted_iota(jnp.int32, (8, LANES), 1)
        tile = zero
        for n, (i, j) in enumerate(pairs):
            value = jnp.sum(sums[n], axis=(0, 1), keepdims=True)
            tile = jnp.where((row == i) & (col == j), value, tile)
        return tile

    def a_copy(i, slot):
        return pltpu.make_async_remote_copy(
            src_ref=coef_a.at[slot], dst_ref=coef_a.at[slot],
            send_sem=ca_send.at[i], recv_sem=ca_recv.at[slot],
            device_id={"tensor": (tensor + i) % tensor_size},
            device_id_type=pl.DeviceIdType.MESH,
        )

    def b_copy(i, slot):
        return pltpu.make_async_remote_copy(
            src_ref=coef_b.at[slot], dst_ref=coef_b.at[slot],
            send_sem=cb_send.at[i], recv_sem=cb_recv.at[slot],
            device_id={"dp": (dp + i) % dp_size}, device_id_type=pl.DeviceIdType.MESH,
        )

    loads[0].wait()
    loads[1].wait()
    for i in range(1, ys):
        make((y + i) % ys)
    loads[2].wait()
    y_start(tensor)
    make(y)
    for i in range(1, ys):
        arrive(partner, (y + i) % ys)
    y_start(partner)
    keep(tensor)
    arrive(partner, y)
    keep(partner)

    for load in loads[3:]:
        load.wait()
    coef_a[tensor] = coef_partial()
    for i in range(1, tensor_size):
        a_copy(i, tensor).start()

    for n in range(1, xs):
        other = (x + n) % xs
        for i in range(1, ys):
            arrive(other * 2 + core, (y + i) % ys)
            to_partner(other * 2 + core, (y + i) % ys).start()
        y_start(other * 2 + core)
        for i in range(1, ys):
            arrive(other * 2 + 1 - core, (y + i) % ys)
        y_start(other * 2 + 1 - core)

    pass_on(tensor)
    for i in range(1, tensor_size):
        a_copy(i, (tensor + tensor_size - i) % tensor_size).wait_recv()
    total = coef_a[0]
    for i in range(1, tensor_size):
        total += coef_a[i]
    coef_b[dp] = total
    for i in range(1, dp_size):
        b_copy(i, dp).start()
    pass_on(partner)

    for n in range(1, xs):
        other = (x + n) % xs
        arrive(other * 2 + core, y)
        to_partner(other * 2 + core, y).start()
        keep(other * 2 + core)
        arrive(other * 2 + 1 - core, y)
        keep(other * 2 + 1 - core)
        pass_on(other * 2 + core)
        pass_on(other * 2 + 1 - core)

    for i in range(1, dp_size):
        b_copy(i, (dp + dp_size - i) % dp_size).wait_recv()
    total = coef_b[0]
    for i in range(1, dp_size):
        total += coef_b[i]
    coef_out[...] = total[: coef_out.shape[0], : coef_out.shape[1]]

    @pl.loop(0, CHUNKS)
    def _(k):
        proj_out[strip(k), :] = own[z, strip(k), :]

        @pl.when(z > 0)
        def _():
            right_copy(z, k).wait_recv()
            proj_out[strip(k), :] += z_left[z, strip(k), :].astype(jnp.float32)

        @pl.when(z < zs - 1)
        def _():
            left_copy(z, k).wait_recv()
            proj_out[strip(k), :] += z_right[z, strip(k), :].astype(jnp.float32)

    for slot in range(zs):
        @pl.when(slot != z)
        def _():
            @pl.loop(0, CHUNKS)
            def _(k):
                right_copy(slot, k).wait_send()

    for part in range(ys):
        for n in range(xs):
            to_partner(n * 2 + core, part).wait_send()
        for n in range(1, xs):
            to_x((x + n) % xs, part).wait_send()
    for i in range(1, tensor_size):
        a_copy(i, tensor).wait_send()
    for i in range(1, dp_size):
        b_copy(i, dp).wait_send()


def local(dp_size, tensor_size, layer_outs, avg_grads, attn_mixed, dwa_coefs):
    depth, tokens, features = avg_grads.shape
    rows = features * tensor_size // dp_size
    cols = attn_mixed.shape[1]
    ys, zs, xs = dp_size // tensor_size, tensor_size, tensor_size // 2
    bf16, f32 = jnp.bfloat16, jnp.float32
    dma = pltpu.SemaphoreType.DMA
    any_space = pl.BlockSpec(memory_space=pl.ANY)
    vmem = pl.BlockSpec(memory_space=pltpu.VMEM)
    return pl.pallas_call(
        functools.partial(kernel, dp_size, tensor_size),
        out_shape=(
            jax.ShapeDtypeStruct(dwa_coefs.shape, f32),
            jax.ShapeDtypeStruct((rows, cols), f32),
        ),
        in_specs=[any_space, any_space, any_space, pl.BlockSpec(memory_space=pltpu.SMEM)],
        out_specs=(vmem, vmem),
        scratch_shapes=[
            pltpu.VMEM(layer_outs.shape, bf16),
            pltpu.VMEM(avg_grads.shape, bf16),
            pltpu.VMEM(attn_mixed.shape, bf16),
            pltpu.VMEM((tensor_size, features, tokens), bf16),
            pltpu.VMEM((ys - 1, zs, rows, cols), bf16),
            pltpu.VMEM((ys - 1, zs, rows, cols), bf16),
            pltpu.VMEM((zs, rows, cols), f32),
            pltpu.VMEM((zs, rows, cols), bf16),
            pltpu.VMEM((zs, rows, cols), bf16),
            pltpu.VMEM((tensor_size, 8, LANES), f32),
            pltpu.VMEM((dp_size, 8, LANES), f32),
            dma((2 * depth + 2,)),
            dma((xs, ys)),
            dma((xs, ys)),
            dma((tensor_size, ys)),
            dma((ys - 1, zs, CHUNKS)),
            dma((ys - 1, zs, CHUNKS)),
            dma((zs, CHUNKS)),
            dma((zs, CHUNKS)),
            dma((zs, CHUNKS)),
            dma((tensor_size,)),
            dma((tensor_size,)),
            dma((dp_size,)),
            dma((dp_size,)),
        ],
        compiler_params=pltpu.CompilerParams(
            collective_id=0, has_side_effects=True, vmem_limit_bytes=67000000
        ),
    )(layer_outs, avg_grads, attn_mixed, dwa_coefs)


def solution(mesh):
    sizes = (mesh.shape["dp"], mesh.shape["tensor"])
    in_specs = (P(None, "dp", "tensor"), P(None, "dp", "tensor"), P("dp", "tensor"), P())
    out_specs = (P(), P("dp", "tensor"))
    return jax.shard_map(
        functools.partial(local, *sizes), mesh=mesh, in_specs=in_specs, out_specs=out_specs, check_vma=False
    )
```

```python
import functools

import jax
import jax.numpy as jnp
from jax import lax
from jax.experimental import pallas as pl
from jax.experimental.pallas import tpu as pltpu
from jax.sharding import PartitionSpec as P

CHUNKS = 8
GROUP = 4
LANES = 128


def kernel(
    dp_size, tensor_size, outs_hbm, grads_hbm, attn_hbm, coefs, coef_out, proj_out,
    outs, grads, attn, gathered, y_send, y_recv, own, z_left, z_right, coef_a, coef_b,
    load_sem, g_send, x_send, g_recv, y_send_sem, y_recv_sem,
    z_send_sem, zl_sem, zr_sem, ca_send, ca_recv, cb_send, cb_recv,
):
    depth, tokens, features = grads.shape
    rows, cols = proj_out.shape
    ys = dp_size // tensor_size
    zs = tensor_size
    xs = tensor_size // 2
    chunk = rows // CHUNKS
    dp, tensor = lax.axis_index("dp"), lax.axis_index("tensor")
    z, y = dp // ys, dp % ys
    x, core = tensor // 2, tensor % 2
    partner = x * 2 + 1 - core

    loads = []
    order = [depth - 2, depth - 1]
    for i in order:
        loads.append(pltpu.make_async_copy(grads_hbm.at[i], grads.at[i], load_sem.at[i]))
    loads.append(pltpu.make_async_copy(attn_hbm, attn, load_sem.at[depth]))
    for i in range(depth - 2):
        loads.append(pltpu.make_async_copy(grads_hbm.at[i], grads.at[i], load_sem.at[i]))
    for j in range(depth + 1):
        loads.append(pltpu.make_async_copy(outs_hbm.at[j], outs.at[j], load_sem.at[depth + 1 + j]))
    for load in loads[:3]:
        load.start()

    barrier = pltpu.get_barrier_semaphore()
    for i in range(1, tensor_size):
        pl.semaphore_signal(
            barrier, inc=1, device_id={"tensor": (tensor + i) % tensor_size},
            device_id_type=pl.DeviceIdType.MESH,
        )
    for i in range(1, dp_size):
        pl.semaphore_signal(
            barrier, inc=1, device_id={"dp": (dp + i) % dp_size},
            device_id_type=pl.DeviceIdType.MESH,
        )
    pl.semaphore_wait(barrier, tensor_size + dp_size - 2)

    def piece(slot, part):
        return gathered.at[slot, pl.ds(pl.multiple_of(part * rows, rows), rows), :]

    def to_partner(slot, part):
        return pltpu.make_async_remote_copy(
            src_ref=piece(slot, part), dst_ref=piece(slot, part),
            send_sem=g_send.at[slot // 2, part], recv_sem=g_recv.at[slot, part],
            device_id={"tensor": partner}, device_id_type=pl.DeviceIdType.MESH,
        )

    def to_x(other, part):
        return pltpu.make_async_remote_copy(
            src_ref=piece(tensor, part), dst_ref=piece(tensor, part),
            send_sem=x_send.at[other, part], recv_sem=g_recv.at[tensor, part],
            device_id={"tensor": other * 2 + core}, device_id_type=pl.DeviceIdType.MESH,
        )

    def arrive(slot, part):
        pltpu.make_async_remote_copy(
            src_ref=piece(slot, part), dst_ref=piece(slot, part),
            send_sem=g_send.at[slot // 2, part], recv_sem=g_recv.at[slot, part],
            device_id={"tensor": partner}, device_id_type=pl.DeviceIdType.MESH,
        ).wait_recv()

    def make(part):
        first, second = coefs[depth - 2, depth - 1], coefs[depth - 1, depth - 1]

        @pl.loop(0, tokens // LANES)
        def _(step):
            at = pl.ds(pl.multiple_of(step * LANES, LANES), LANES)
            wide = pl.ds(pl.multiple_of(part * rows, LANES), rows)
            value = first * grads[depth - 2, at, wide].astype(jnp.float32)
            value += second * grads[depth - 1, at, wide].astype(jnp.float32)
            into = pl.ds(pl.multiple_of(part * rows, rows), rows)
            gathered[tensor, into, at] = value.T.astype(jnp.bfloat16)

        to_partner(tensor, part).start()
        for i in range(1, xs):
            to_x((x + i) % xs, part).start()

    def block(slot, part, k):
        at = pl.ds(pl.multiple_of(part * rows + k * chunk, chunk), chunk * GROUP)
        return jnp.dot(gathered[slot, at, :], attn[...], preferred_element_type=jnp.float32)

    def strip(k, count=1):
        return pl.ds(pl.multiple_of(k * chunk, chunk), chunk * count)

    def y_copy(slot, i, k):
        return pltpu.make_async_remote_copy(
            src_ref=y_send.at[i - 1, slot, strip(k), :], dst_ref=y_recv.at[i - 1, slot, strip(k), :],
            send_sem=y_send_sem.at[i - 1, slot, k], recv_sem=y_recv_sem.at[i - 1, slot, k],
            device_id={"dp": z * ys + (y + i) % ys}, device_id_type=pl.DeviceIdType.MESH,
        )

    def y_start(slot):
        for i in range(1, ys):
            @pl.loop(0, CHUNKS // GROUP)
            def _(g):
                k = g * GROUP
                value = block(slot, (y + i) % ys, k)
                y_send[i - 1, slot, strip(k, GROUP), :] = value.astype(jnp.bfloat16)
                for n in range(GROUP):
                    y_copy(slot, i, k + n).start()

    def keep(slot):
        @pl.loop(0, CHUNKS // GROUP)
        def _(g):
            k = g * GROUP
            own[slot, strip(k, GROUP), :] = block(slot, y, k)

    def right_copy(slot, k):
        return pltpu.make_async_remote_copy(
            src_ref=y_send.at[0, slot, strip(k), :], dst_ref=z_left.at[slot, strip(k), :],
            send_sem=z_send_sem.at[slot, k], recv_sem=zl_sem.at[slot, k],
            device_id={"dp": dp + ys}, device_id_type=pl.DeviceIdType.MESH,
        )

    def left_copy(slot, k):
        return pltpu.make_async_remote_copy(
            src_ref=y_send.at[0, slot, strip(k), :], dst_ref=z_right.at[slot, strip(k), :],
            send_sem=z_send_sem.at[slot, k], recv_sem=zr_sem.at[slot, k],
            device_id={"dp": dp - ys}, device_id_type=pl.DeviceIdType.MESH,
        )

    def pass_on(slot):
        @pl.loop(0, CHUNKS)
        def _(k):
            total = own[slot, strip(k), :]
            for i in range(1, ys):
                y_copy(slot, i, k).wait_send()
                y_copy(slot, i, k).wait_recv()
                total += y_recv[i - 1, slot, strip(k), :].astype(jnp.float32)
            own[slot, strip(k), :] = total

            @pl.when(slot > z)
            def _():
                @pl.when(z > 0)
                def _():
                    right_copy(slot, k).wait_recv()
                    own[slot, strip(k), :] += z_left[slot, strip(k), :].astype(jnp.float32)

                y_send[0, slot, strip(k), :] = own[slot, strip(k), :].astype(jnp.bfloat16)
                right_copy(slot, k).start()

            @pl.when(slot < z)
            def _():
                @pl.when(z < zs - 1)
                def _():
                    left_copy(slot, k).wait_recv()
                    own[slot, strip(k), :] += z_right[slot, strip(k), :].astype(jnp.float32)

                y_send[0, slot, strip(k), :] = own[slot, strip(k), :].astype(jnp.bfloat16)
                left_copy(slot, k).start()

    def coef_partial():
        pairs = [(i, j) for i in range(depth) for j in range(min(i + 2, depth + 1))]

        def step(r, sums):
            at = pl.ds(pl.multiple_of(r * 16, 16), 16)
            sums = list(sums)
            for col in range(features // LANES):
                lanes = slice(col * LANES, (col + 1) * LANES)
                g = [grads[i, at, lanes].astype(jnp.float32) for i in range(depth)]
                o = [outs[j, at, lanes].astype(jnp.float32) for j in range(depth + 1)]
                for n, (i, j) in enumerate(pairs):
                    product = g[i] * o[j]
                    sums[n] += product[:8] + product[8:]
            return tuple(sums)

        zero = jnp.zeros((8, LANES), jnp.float32)
        sums = lax.fori_loop(0, tokens // 16, step, tuple(zero for _ in pairs))
        row = lax.broadcasted_iota(jnp.int32, (8, LANES), 0)
        col = lax.broadcasted_iota(jnp.int32, (8, LANES), 1)
        tile = zero
        for n, (i, j) in enumerate(pairs):
            value = jnp.sum(sums[n], axis=(0, 1), keepdims=True)
            tile = jnp.where((row == i) & (col == j), value, tile)
        return tile

    def a_copy(i, slot):
        return pltpu.make_async_remote_copy(
            src_ref=coef_a.at[slot], dst_ref=coef_a.at[slot],
            send_sem=ca_send.at[i], recv_sem=ca_recv.at[slot],
            device_id={"tensor": (tensor + i) % tensor_size},
            device_id_type=pl.DeviceIdType.MESH,
        )

    def b_copy(i, slot):
        return pltpu.make_async_remote_copy(
            src_ref=coef_b.at[slot], dst_ref=coef_b.at[slot],
            send_sem=cb_send.at[i], recv_sem=cb_recv.at[slot],
            device_id={"dp": (dp + i) % dp_size}, device_id_type=pl.DeviceIdType.MESH,
        )

    loads[0].wait()
    loads[1].wait()
    for i in range(1, ys):
        make((y + i) % ys)
    loads[2].wait()
    y_start(tensor)
    for load in loads[3:]:
        load.start()
    make(y)
    for i in range(1, ys):
        arrive(partner, (y + i) % ys)
    y_start(partner)
    keep(tensor)
    arrive(partner, y)
    keep(partner)

    for load in loads[3:]:
        load.wait()
    coef_a[tensor] = coef_partial()
    for i in range(1, tensor_size):
        a_copy(i, tensor).start()

    others = []
    for n in range(1, xs):
        other = (x + n) % xs
        far = jnp.where(other < xs // 2, other * 2, other * 2 + 1)
        others.append((other, far, other * 4 + 1 - far))

    for other, far, near in others:
        for i in range(1, ys):
            arrive(other * 2 + core, (y + i) % ys)
            to_partner(other * 2 + core, (y + i) % ys).start()
        for i in range(1, ys):
            arrive(other * 2 + 1 - core, (y + i) % ys)
        y_start(far)
        y_start(near)

    pass_on(tensor)
    for i in range(1, tensor_size):
        a_copy(i, (tensor + tensor_size - i) % tensor_size).wait_recv()
    total = coef_a[0]
    for i in range(1, tensor_size):
        total += coef_a[i]
    coef_b[dp] = total
    for i in range(1, dp_size):
        b_copy(i, dp).start()

    for other, far, near in others:
        arrive(other * 2 + core, y)
        to_partner(other * 2 + core, y).start()
        arrive(other * 2 + 1 - core, y)
        keep(far)
        keep(near)
    pass_on(partner)
    for other, far, near in others:
        pass_on(far)
        pass_on(near)

    for i in range(1, dp_size):
        b_copy(i, (dp + dp_size - i) % dp_size).wait_recv()
    total = coef_b[0]
    for i in range(1, dp_size):
        total += coef_b[i]
    coef_out[...] = total[: coef_out.shape[0], : coef_out.shape[1]]

    @pl.loop(0, CHUNKS)
    def _(k):
        proj_out[strip(k), :] = own[z, strip(k), :]

        @pl.when(z > 0)
        def _():
            right_copy(z, k).wait_recv()
            proj_out[strip(k), :] += z_left[z, strip(k), :].astype(jnp.float32)

        @pl.when(z < zs - 1)
        def _():
            left_copy(z, k).wait_recv()
            proj_out[strip(k), :] += z_right[z, strip(k), :].astype(jnp.float32)

    for slot in range(zs):
        @pl.when(slot != z)
        def _():
            @pl.loop(0, CHUNKS)
            def _(k):
                right_copy(slot, k).wait_send()

    for part in range(ys):
        for n in range(xs):
            to_partner(n * 2 + core, part).wait_send()
        for n in range(1, xs):
            to_x((x + n) % xs, part).wait_send()
    for i in range(1, tensor_size):
        a_copy(i, tensor).wait_send()
    for i in range(1, dp_size):
        b_copy(i, dp).wait_send()


def local(dp_size, tensor_size, layer_outs, avg_grads, attn_mixed, dwa_coefs):
    depth, tokens, features = avg_grads.shape
    rows = features * tensor_size // dp_size
    cols = attn_mixed.shape[1]
    ys, zs, xs = dp_size // tensor_size, tensor_size, tensor_size // 2
    bf16, f32 = jnp.bfloat16, jnp.float32
    dma = pltpu.SemaphoreType.DMA
    any_space = pl.BlockSpec(memory_space=pl.ANY)
    vmem = pl.BlockSpec(memory_space=pltpu.VMEM)
    return pl.pallas_call(
        functools.partial(kernel, dp_size, tensor_size),
        out_shape=(
            jax.ShapeDtypeStruct(dwa_coefs.shape, f32),
            jax.ShapeDtypeStruct((rows, cols), f32),
        ),
        in_specs=[any_space, any_space, any_space, pl.BlockSpec(memory_space=pltpu.SMEM)],
        out_specs=(vmem, vmem),
        scratch_shapes=[
            pltpu.VMEM(layer_outs.shape, bf16),
            pltpu.VMEM(avg_grads.shape, bf16),
            pltpu.VMEM(attn_mixed.shape, bf16),
            pltpu.VMEM((tensor_size, features, tokens), bf16),
            pltpu.VMEM((ys - 1, zs, rows, cols), bf16),
            pltpu.VMEM((ys - 1, zs, rows, cols), bf16),
            pltpu.VMEM((zs, rows, cols), f32),
            pltpu.VMEM((zs, rows, cols), bf16),
            pltpu.VMEM((zs, rows, cols), bf16),
            pltpu.VMEM((tensor_size, 8, LANES), f32),
            pltpu.VMEM((dp_size, 8, LANES), f32),
            dma((2 * depth + 2,)),
            dma((xs, ys)),
            dma((xs, ys)),
            dma((tensor_size, ys)),
            dma((ys - 1, zs, CHUNKS)),
            dma((ys - 1, zs, CHUNKS)),
            dma((zs, CHUNKS)),
            dma((zs, CHUNKS)),
            dma((zs, CHUNKS)),
            dma((tensor_size,)),
            dma((tensor_size,)),
            dma((dp_size,)),
            dma((dp_size,)),
        ],
        compiler_params=pltpu.CompilerParams(
            collective_id=0, has_side_effects=True, vmem_limit_bytes=67000000
        ),
    )(layer_outs, avg_grads, attn_mixed, dwa_coefs)


def solution(mesh):
    sizes = (mesh.shape["dp"], mesh.shape["tensor"])
    in_specs = (P(None, "dp", "tensor"), P(None, "dp", "tensor"), P("dp", "tensor"), P())
    out_specs = (P(), P("dp", "tensor"))
    return jax.shard_map(
        functools.partial(local, *sizes), mesh=mesh, in_specs=in_specs, out_specs=out_specs, check_vma=False
    )
```
